32 devices in a mesh: lat: 4 (over z), lon: 8 (over y, x, core).
Axes of the slice: x: 2, y: 2, z: 4, core: 2. Of those that a mesh axis runs over, the one named last changes fastest.
Arguments:
- increments: bfloat16 [65536, 3, 128], P(('lat', 'lon')), may hold values from -6 to 6
- cotangent: bfloat16 [65536, 128], P(('lat', 'lon')), may hold values from -6 to 6
- owner_perm: int32 [32, 2048], P(('lat', 'lon')), may hold values from 0 to 2047, each once within a row
- coarse_index: int32 [2, 32768], P(None, ('lat', 'lon')), may hold values from 0 to 2047
- coarse_weight: float32 [32768], P(('lat', 'lon')), may hold values from 0.2 to 0.8
- back_index: int32 [2, 65536], P(None, ('lat', 'lon')), may hold values from 0 to 1023
- back_weight: float32 [65536], P(('lat', 'lon')), may hold values from 0.2 to 0.8
- lw_scale: float32 [16, 32768], P(None, ('lat', 'lon')), may hold values from 0.1 to 1
- sw_scale: float32 [14, 32768], P(None, ('lat', 'lon')), may hold values from 0.2 to 2
- sunlit: int32 [32768], P(('lat', 'lon')), may hold values from 0 to 1, as said below
- lw_table: bfloat16 [16, 3, 128, 128], P(None, None, 'lon'), may hold values from -0.3125 to 0.3125
- sw_table: bfloat16 [14, 3, 128, 128], P(None, None, 'lon'), may hold values from -0.3125 to 0.3125
Outputs:
- tendency: bfloat16 [65536, 128], P(('lat', 'lon'))
- gradient: bfloat16 [65536, 3, 128], P(('lat', 'lon'))
The draws below stay inside these ranges and needn't reach their ends.
Inputs may be any that keep to these rules, and one draw needn't show every extreme that they name: In each device's block of 1024 radiation columns at most 640 are sunlit, and some device has exactly 640.
All inputs are finite; a program needn't handle non-finite values.
Results may differ from the reference program's by a relative error of at most 0.014.
Values may be sent and summed in bfloat16 or wider, within the bound.
A program may use at most 64 MiB of HBM per device.

```python
import math
import jax
import jax.numpy as jnp
from jax import lax

COLS_DEV = 2048
LEV = 128
VARS = 3
BANDS_LW = 16
BANDS_SW = 14
RC_DEV = 1024
SUNMAX = 640
COLS = 65536
RCOLS = 32768
N_LAT = 4
N_LON = 8
DEVICES = 32


def draw_sunlit(key, part):
    key_count, key_full, key_order = jax.random.split(key, 3)
    counts = jax.random.randint(key_count, (DEVICES,), SUNMAX // 8, SUNMAX + 1)
    chosen = jax.random.randint(key_full, (), 0, DEVICES)
    counts = jnp.where(jnp.arange(DEVICES) == chosen, SUNMAX, counts)
    scores = jax.random.randint(key_order, (DEVICES, RC_DEV), 0, 1 << 18) * RC_DEV + jnp.arange(RC_DEV, dtype=jnp.int32)[None, :]
    ranks = jnp.argsort(jnp.argsort(scores, axis=1), axis=1)
    return (ranks < counts[:, None]).astype(jnp.int32).reshape(-1)


def place_ends(values, own_key, smallest, top_value):
    dims = values.shape
    spot = [jax.random.randint(jax.random.fold_in(own_key, axis), (), 0, dims[axis]) for axis in range(len(dims))]
    values = values.at[tuple(spot)].set(smallest)
    longest = dims.index(max(dims))
    spot[longest] = (spot[longest] + 1) % dims[longest]
    return values.at[tuple(spot)].set(top_value)


def block_levels(own_key, shape, cuts, low, high):
    factor_of, own = 1.0, jax.random.fold_in(own_key, 6)
    for axis_at, shards_of in cuts:
        heights = jnp.exp(jax.random.uniform(jax.random.fold_in(own, axis_at), (shards_of,), jnp.float32, low / len(cuts), high / len(cuts)))
        factor_of = factor_of * jnp.repeat(heights, shape[axis_at] // shards_of).reshape([-1 if axis == axis_at else 1 for axis in range(len(shape))])
    return factor_of


def scatter_about(stream_key, shape, deviation, bound, cuts=(), kind=jnp.bfloat16):
    array = jax.random.normal(stream_key, shape, jnp.float32) * deviation
    if len(cuts) > 0:
        array = block_levels(stream_key, shape, cuts, -0.22, 0.18) * array
    return jnp.clip(array, min=-bound, max=bound).astype(kind)


def setup_inputs(seed: int = 0) -> dict:
    splits = jax.random.split(jax.random.key(seed), 13)
    increments = scatter_about(splits[0], (COLS, VARS, LEV), 1.0, 6.0, ((0, 32),))
    cotangent = scatter_about(splits[1], (COLS, LEV), 1.0, 6.0, ((0, 32),))
    owner_perm = jax.vmap(lambda own: jax.random.permutation(own, COLS_DEV))(jax.random.split(splits[2], DEVICES)).reshape((DEVICES, COLS_DEV)).astype(jnp.int32)
    coarse_index = place_ends(jax.random.randint(splits[3], (2, RCOLS), 0, COLS_DEV), jax.random.fold_in(splits[3], 1), 0, COLS_DEV - 1).astype(jnp.int32)
    coarse_weight = jnp.clip(0.2 + 0.6 * jax.random.uniform(splits[4], (RCOLS,), jnp.float32) ** block_levels(splits[4], (RCOLS,), ((0, 32),), -0.2, 0.2), 0.2, 0.8)
    back_index = place_ends(jax.random.randint(splits[5], (2, COLS), 0, RC_DEV), jax.random.fold_in(splits[5], 1), 0, RC_DEV - 1).astype(jnp.int32)
    back_weight = jnp.clip(0.2 + 0.6 * jax.random.uniform(splits[6], (COLS,), jnp.float32) ** block_levels(splits[6], (COLS,), ((0, 32),), -0.2, 0.2), 0.2, 0.8)
    lw_scale = jnp.clip(jnp.exp(math.log(1.0) - 2.3025851 * jax.random.uniform(splits[7], (BANDS_LW, RCOLS), jnp.float32) ** block_levels(splits[7], (BANDS_LW, RCOLS), ((1, 32),), -0.2, 0.2)), 0.1, 1.0)
    sw_scale = jnp.clip(jnp.exp(math.log(2.0) - 2.3025851 * jax.random.uniform(splits[8], (BANDS_SW, RCOLS), jnp.float32) ** block_levels(splits[8], (BANDS_SW, RCOLS), ((1, 32),), -0.2, 0.2)), 0.2, 2.0)
    sunlit = draw_sunlit(jax.random.fold_in(splits[12], 71), 0)
    lw_table = scatter_about(splits[10], (BANDS_LW, VARS, LEV, LEV), (VARS * LEV) ** -0.5, 0.3125, ((2, 8),))
    sw_table = scatter_about(splits[11], (BANDS_SW, VARS, LEV, LEV), (VARS * LEV) ** -0.5, 0.3125, ((2, 8),))
    return {"increments": increments, "cotangent": cotangent, "owner_perm": owner_perm, "coarse_index": coarse_index, "coarse_weight": coarse_weight, "back_index": back_index, "back_weight": back_weight, "lw_scale": lw_scale, "sw_scale": sw_scale, "sunlit": sunlit, "lw_table": lw_table, "sw_table": sw_table}


def band_sum(coarse, band_table, band_scale):
    product = jnp.einsum("rc,bck->rbk", coarse.astype(jnp.float32), band_table.astype(jnp.float32))
    return jnp.einsum("br,rbk->rk", band_scale, product)


def band_adjoint(adjoint_coarse, band_table, band_scale):
    lifted = (band_scale.T[:, :, None] * adjoint_coarse[:, None, :]).astype(jnp.bfloat16)
    lifted = lax.optimization_barrier(lifted)
    return jnp.einsum("rbk,bck->rc", lifted.astype(jnp.float32), band_table.astype(jnp.float32))


def radiate(fields, cot_rad, coarse_index, coarse_weight, back_index, back_weight, lw_scale, sw_scale, sunlit, lw_bands, sw_bands):
    row_count = coarse_weight.shape[0]
    col_count = back_weight.shape[0]
    flat_rows = fields.reshape(col_count, -1)
    first = flat_rows[coarse_index[0]].astype(jnp.float32)
    second = flat_rows[coarse_index[1]].astype(jnp.float32)
    coarse = (coarse_weight[:, None] * first + (1.0 - coarse_weight)[:, None] * second).astype(jnp.bfloat16)
    sw_weight = sw_scale * sunlit.astype(jnp.float32)[None, :]
    heating = band_sum(coarse, lw_bands, lw_scale) + band_sum(coarse, sw_bands, sw_weight)
    tendency_rad = (back_weight[:, None] * heating[back_index[0]] + (1.0 - back_weight)[:, None] * heating[back_index[1]]).astype(jnp.bfloat16)
    cot_float = cot_rad.astype(jnp.float32)
    adjoint_coarse = jax.ops.segment_sum(
        jnp.concatenate([back_weight[:, None] * cot_float, (1.0 - back_weight)[:, None] * cot_float]),
        jnp.concatenate([back_index[0], back_index[1]]), num_segments=row_count)
    adjoint_rows = band_adjoint(adjoint_coarse, lw_bands, lw_scale) + band_adjoint(adjoint_coarse, sw_bands, sw_weight)
    gradient_rad = jax.ops.segment_sum(
        jnp.concatenate([coarse_weight[:, None] * adjoint_rows, (1.0 - coarse_weight)[:, None] * adjoint_rows]),
        jnp.concatenate([coarse_index[0], coarse_index[1]]), num_segments=col_count).astype(jnp.bfloat16)
    return tendency_rad, gradient_rad.reshape(fields.shape)


def pick_rows(values, order_map):
    return values[order_map]


def restore_rows(values, order_map):
    return jnp.zeros_like(values).at[order_map].set(values)


def reference(increments, cotangent, owner_perm, coarse_index, coarse_weight, back_index, back_weight, lw_scale, sw_scale, sunlit, lw_table, sw_table):
    device_count = N_LAT * N_LON
    segment = COLS_DEV // device_count

    def relay(values):
        rest = values.shape[2:]
        return values.reshape((device_count, device_count, segment) + rest).swapaxes(0, 1).reshape((device_count, COLS_DEV) + rest)

    fields_model = increments.reshape(device_count, COLS_DEV, VARS, LEV)
    cot_model = cotangent.reshape(device_count, COLS_DEV, LEV)
    fields = relay(jax.vmap(pick_rows)(fields_model, owner_perm))
    cot_rad = relay(jax.vmap(pick_rows)(cot_model, owner_perm))
    coarse_dev = coarse_index.reshape(2, device_count, RC_DEV).swapaxes(0, 1)
    coarse_wdev = coarse_weight.reshape(device_count, RC_DEV)
    back_dev = back_index.reshape(2, device_count, COLS_DEV).swapaxes(0, 1)
    back_wdev = back_weight.reshape(device_count, COLS_DEV)
    lw_dev = lw_scale.reshape(BANDS_LW, device_count, RC_DEV).swapaxes(0, 1)
    sw_dev = sw_scale.reshape(BANDS_SW, device_count, RC_DEV).swapaxes(0, 1)
    sun_dev = sunlit.reshape(device_count, RC_DEV)
    lw_bands = lw_table.reshape(BANDS_LW, VARS * LEV, LEV)
    sw_bands = sw_table.reshape(BANDS_SW, VARS * LEV, LEV)

    def one_device(item):
        return radiate(item[0], item[1], item[2], item[3], item[4], item[5], item[6], item[7], item[8], lw_bands, sw_bands)

    tendency_rad, gradient_rad = lax.map(one_device, (fields, cot_rad, coarse_dev, coarse_wdev, back_dev, back_wdev, lw_dev, sw_dev, sun_dev))
    tendency = jax.vmap(restore_rows)(relay(tendency_rad), owner_perm)
    gradient = jax.vmap(restore_rows)(relay(gradient_rad), owner_perm)
    return tendency.reshape(COLS, LEV), gradient.reshape(COLS, VARS, LEV)
```

```python
import jax
import jax.numpy as jnp
from jax import lax
from jax.experimental import pallas as pl
from jax.experimental.pallas import tpu as pltpu
from jax.sharding import PartitionSpec as P

BLOCK = 256


def lane_iota(rows, width):
    return lax.broadcasted_iota(jnp.int32, (rows, width), 1)


def row_iota(rows, width, start):
    return lax.broadcasted_iota(jnp.int32, (rows, width), 0) + start


def pick(hit):
    return jnp.where(hit, 1.0, 0.0).astype(jnp.bfloat16)


def blend(hit_first, hit_second, share):
    first = jnp.where(hit_first, share, 0.0)
    second = jnp.where(hit_second, 1.0 - share, 0.0)
    return (first + second).astype(jnp.bfloat16)


def dot(left, right):
    return lax.dot_general(left, right, (((1,), (0,)), ((), ())), preferred_element_type=jnp.float32)


def send_kernel(perm_ref, inc_ref, cot_ref, cot_out, fields_out, stacked):
    var_count, col_count, width = inc_ref.shape
    segment = fields_out.shape[2]
    per_block = BLOCK // segment
    stacked[:, pl.ds(0, width)] = cot_ref[...]
    for v in range(var_count):
        stacked[:, pl.ds((v + 1) * width, width)] = inc_ref[v]

    @pl.loop(0, col_count // BLOCK)
    def one(step):
        rows = pl.ds(pl.multiple_of(step * BLOCK, BLOCK), BLOCK)
        column = jnp.transpose(jnp.broadcast_to(perm_ref[:, rows], (8, BLOCK)))[:, 0:1]
        table = pick(column == lane_iota(BLOCK, col_count))
        moved = dot(table, stacked[...]).astype(jnp.bfloat16)
        cot_out[rows, :] = moved[:, :width]
        for v in range(var_count):
            piece = moved[:, (v + 1) * width : (v + 2) * width]
            fields_out[pl.ds(step * per_block, per_block), v] = piece.reshape(per_block, segment, width)


def lay_tables(lw_ref, sw_ref, wide):
    at = 0
    for ref in (lw_ref, sw_ref):
        for b in range(ref.shape[0]):
            wide[:, pl.ds(at, ref.shape[3])] = ref[b].reshape(wide.shape[0], ref.shape[3])
            at += ref.shape[3]


def adjoint_kernel(cot_ref, back_ref, back_w, scale_ref, lw_ref, sw_ref, coarse_ref, coarse_w, grad_out, wide_out, adj):
    lay_tables(lw_ref, sw_ref, wide_out)
    row_count = scale_ref.shape[1]
    col_count, width = cot_ref.shape
    band_count = lw_ref.shape[0] + sw_ref.shape[0]
    var_count, segment = grad_out.shape[1], grad_out.shape[2]
    per_block = BLOCK // segment

    @pl.loop(0, row_count // BLOCK)
    def one(step):
        start = pl.multiple_of(step * BLOCK, BLOCK)
        rows = pl.ds(start, BLOCK)
        spot = row_iota(BLOCK, col_count, start)
        table = blend(back_ref[0:1, :] == spot, back_ref[1:2, :] == spot, back_w[...])
        coarse = dot(table, cot_ref[...])
        scale = jnp.transpose(scale_ref[:, rows])
        lifted = jnp.concatenate([(scale[:, b : b + 1] * coarse).astype(jnp.bfloat16) for b in range(band_count)], axis=1)
        out = lax.dot_general(lifted, wide_out[...], (((1,), (1,)), ((), ())), preferred_element_type=jnp.float32)
        adj[rows, :] = out.astype(jnp.bfloat16)

    @pl.loop(0, col_count // BLOCK)
    def two(step):
        spot = row_iota(BLOCK, row_count, step * BLOCK)
        table = blend(coarse_ref[0:1, :] == spot, coarse_ref[1:2, :] == spot, coarse_w[...])
        moved = dot(table, adj[...]).astype(jnp.bfloat16)
        for v in range(var_count):
            piece = moved[:, v * width : (v + 1) * width]
            grad_out[pl.ds(step * per_block, per_block), v] = piece.reshape(per_block, segment, width)


def column_of(values):
    return jnp.transpose(jnp.broadcast_to(values, (8, values.shape[1])))[:, 0:1]


def heating_kernel(fields_ref, back_ref, back_w, scale_ref, wide_ref, coarse_ref, coarse_w, tend_out, flat, heat):
    devices, var_count, segment, width = fields_ref.shape
    col_count = devices * segment
    row_count = scale_ref.shape[1]
    band_count = wide_ref.shape[1] // width
    for v in range(var_count):
        flat[:, pl.ds(v * width, width)] = fields_ref[:, v].reshape(col_count, width)

    @pl.loop(0, row_count // BLOCK)
    def one(step):
        rows = pl.ds(pl.multiple_of(step * BLOCK, BLOCK), BLOCK)
        spot = lane_iota(BLOCK, col_count)
        first, second = column_of(coarse_ref[0:1, rows]), column_of(coarse_ref[1:2, rows])
        table = blend(first == spot, second == spot, column_of(coarse_w[:, rows]))
        coarse = dot(table, flat[...]).astype(jnp.bfloat16)
        scale = jnp.transpose(scale_ref[:, rows])
        total = jnp.zeros((BLOCK, width), jnp.float32)
        for b in range(0, band_count, 2):
            pair = dot(coarse, wide_ref[:, b * width : (b + 2) * width])
            total = total + scale[:, b : b + 1] * pair[:, :width] + scale[:, b + 1 : b + 2] * pair[:, width:]
        heat[rows, :] = total.astype(jnp.bfloat16)

    @pl.loop(0, col_count // BLOCK)
    def two(step):
        rows = pl.ds(pl.multiple_of(step * BLOCK, BLOCK), BLOCK)
        spot = lane_iota(BLOCK, row_count)
        first, second = column_of(back_ref[0:1, rows]), column_of(back_ref[1:2, rows])
        table = blend(first == spot, second == spot, column_of(back_w[:, rows]))
        tend_out[rows, :] = dot(table, heat[...]).astype(jnp.bfloat16)


def restore_kernel(perm_ref, tend_ref, grad_ref, tend_out, grad_out, stacked):
    devices, var_count, segment, width = grad_ref.shape
    col_count = devices * segment
    stacked[:, pl.ds(0, width)] = tend_ref[...]
    for v in range(var_count):
        stacked[:, pl.ds((v + 1) * width, width)] = grad_ref[:, v].reshape(col_count, width)

    @pl.loop(0, col_count // BLOCK)
    def one(step):
        rows = pl.ds(pl.multiple_of(step * BLOCK, BLOCK), BLOCK)
        table = pick(perm_ref[...] == row_iota(BLOCK, col_count, step * BLOCK))
        moved = dot(table, stacked[...]).astype(jnp.bfloat16)
        tend_out[rows, :] = moved[:, :width]
        for v in range(var_count):
            grad_out[v, rows, :] = moved[:, (v + 1) * width : (v + 2) * width]


def run(kernel, outs, scratch, flops, args):
    shapes = [jax.ShapeDtypeStruct(shape, jnp.bfloat16) for shape in outs]
    vmem = pl.BlockSpec(memory_space=pltpu.VMEM)
    return pl.pallas_call(
        kernel,
        out_shape=shapes,
        in_specs=[vmem] * len(args),
        out_specs=[vmem] * len(outs),
        scratch_shapes=[pltpu.VMEM(shape, jnp.bfloat16) for shape in scratch],
        compiler_params=pltpu.CompilerParams(vmem_limit_bytes=56 * 1024 * 1024),
        cost_estimate=pl.CostEstimate(flops=flops, bytes_accessed=4 << 20, transcendentals=0),
    )(*args)


def local(
    increments,
    cotangent,
    owner_perm,
    coarse_index,
    coarse_weight,
    back_index,
    back_weight,
    lw_scale,
    sw_scale,
    sunlit,
    lw_table,
    sw_table,
    *,
    devices,
):
    axes = ("lat", "lon")
    sw_full = lax.all_gather(sw_table, "lon", axis=2, tiled=True)
    lw_full = lax.all_gather(lw_table, "lon", axis=2, tiled=True)
    col_count, var_count, width = increments.shape
    row_count = coarse_weight.shape[0]
    segment = col_count // devices
    split = (devices, var_count, segment, width)
    flat_width = var_count * width
    bands = lw_table.shape[0] + sw_table.shape[0]
    planes = jnp.transpose(increments, (1, 0, 2))
    stack = (col_count, (var_count + 1) * width)
    move_cost = 2 * col_count * stack[0] * stack[1]
    sent_cot, sent_fields = run(
        send_kernel, [(col_count, width), split], [stack], move_cost, (owner_perm, planes, cotangent)
    )
    cot_rad = lax.all_to_all(sent_cot, axes, split_axis=0, concat_axis=0, tiled=True)
    fields = lax.all_to_all(sent_fields, axes, split_axis=0, concat_axis=0, tiled=True)
    scale = jnp.concatenate([lw_scale, sw_scale * sunlit.astype(jnp.float32)[None, :], jnp.zeros((-bands % 8, row_count), jnp.float32)])
    back_w, coarse_w = back_weight[None, :], coarse_weight[None, :]
    band_cost = 3 * row_count * bands * flat_width * width
    sent_grad, wide = run(
        adjoint_kernel,
        [split, (flat_width, bands * width)],
        [(row_count, flat_width)],
        band_cost,
        (cot_rad, back_index, back_w, scale, lw_full, sw_full, coarse_index, coarse_w),
    )
    back_grad = lax.all_to_all(sent_grad, axes, split_axis=0, concat_axis=0, tiled=True)
    (sent_tend,) = run(
        heating_kernel,
        [(col_count, width)],
        [(col_count, flat_width), (row_count, width)],
        band_cost,
        (fields, back_index, back_w, scale, wide, coarse_index, coarse_w),
    )
    back_tend = lax.all_to_all(sent_tend, axes, split_axis=0, concat_axis=0, tiled=True)
    tendency, gradient = run(
        restore_kernel,
        [(col_count, width), (var_count, col_count, width)],
        [stack],
        move_cost,
        (owner_perm, back_tend, back_grad),
    )
    return (tendency, jnp.transpose(gradient, (1, 0, 2)))


def solution(mesh):
    in_specs = (
        P(("lat", "lon"), None, None),
        P(("lat", "lon"), None),
        P(("lat", "lon"), None),
        P(None, ("lat", "lon")),
        P(("lat", "lon")),
        P(None, ("lat", "lon")),
        P(("lat", "lon")),
        P(None, ("lat", "lon")),
        P(None, ("lat", "lon")),
        P(("lat", "lon")),
        P(None, None, "lon", None),
        P(None, None, "lon", None),
    )
    out_specs = (P(("lat", "lon"), None), P(("lat", "lon"), None, None))
    devices = mesh.shape["lat"] * mesh.shape["lon"]

    def body(*args):
        return local(*args, devices=devices)

    return jax.shard_map(body, mesh=mesh, in_specs=in_specs, out_specs=out_specs, check_vma=False)
```

```python
import functools

import jax
import jax.numpy as jnp
from jax import lax
from jax.experimental import pallas as pl
from jax.experimental.pallas import tpu as pltpu
from jax.sharding import PartitionSpec as P

BLOCK = 256


def lane_iota(rows, width):
    return lax.broadcasted_iota(jnp.int32, (rows, width), 1)


def row_iota(rows, width, start):
    return lax.broadcasted_iota(jnp.int32, (rows, width), 0) + start


def pick(hit):
    return jnp.where(hit, 1.0, 0.0).astype(jnp.bfloat16)


def blend(hit_first, hit_second, share):
    first = jnp.where(hit_first, share, 0.0)
    second = jnp.where(hit_second, 1.0 - share, 0.0)
    return (first + second).astype(jnp.bfloat16)


def dot(left, right):
    return lax.dot_general(left, right, (((1,), (0,)), ((), ())), preferred_element_type=jnp.float32)


def column_of(values):
    return jnp.transpose(jnp.broadcast_to(values, (8, values.shape[1])))[:, 0:1]


def radiate_kernel(
    lon_count,
    perm_ref,
    inc_ref,
    cot_ref,
    back_ref,
    back_w,
    scale_ref,
    tab_ref,
    coarse_ref,
    coarse_w,
    tend_in,
    grad_in,
    stacked,
    cot_out,
    cot_in,
    fields_out,
    fields_in,
    grad_out,
    tend_out,
    tabs,
    wide,
    flat,
    adj,
    heat,
    send_sem,
    recv_sem,
    tab_send,
    tab_recv,
):
    var_count, col_count, width = inc_ref.shape
    devices, segment = cot_out.shape[0], cot_out.shape[1]
    row_count = scale_ref.shape[1]
    band_count = tab_ref.shape[0]
    per_block = BLOCK // segment
    blocks = col_count // BLOCK
    lat, lon = lax.axis_index("lat"), lax.axis_index("lon")
    me = lat * lon_count + lon
    parity = lax.rem(lon, 2)
    partner = lon + 1 - 2 * parity
    home = lax.div(me, per_block)

    def table_copy(source, slot, target, sem):
        return pltpu.make_async_remote_copy(
            src_ref=source,
            dst_ref=tabs.at[slot],
            send_sem=sem,
            recv_sem=tab_recv.at[slot],
            device_id=(lat, target),
            device_id_type=pl.DeviceIdType.MESH,
        )

    def copy(kind, source, landing, target, slot):
        return pltpu.make_async_remote_copy(
            src_ref=source,
            dst_ref=landing,
            send_sem=send_sem.at[kind, target],
            recv_sem=recv_sem.at[kind, slot],
            device_id=(lax.div(target, lon_count), lax.rem(target, lon_count)),
            device_id_type=pl.DeviceIdType.MESH,
        )

    def start_block(kind, source, landing, block):
        for k in range(per_block):
            target = block * per_block + k

            @pl.when(target != me)
            def _():
                copy(kind, source.at[target], landing.at[me], target, me).start()

    def wait_all(kind, landing):
        @pl.loop(1, devices)
        def _(k):
            source = lax.rem(me + k, devices)
            copy(kind, landing.at[source], landing.at[source], source, source).wait_recv()

    def wait_sent(kind, source):
        @pl.loop(1, devices)
        def _(k):
            target = lax.rem(me + k, devices)
            copy(kind, source.at[target], source.at[target], target, target).wait_send()

    def turn(step):
        return lax.rem(step + home + 1, blocks)

    def split_rows(ref, block, values):
        for v in range(var_count):
            piece = values[:, v * width : (v + 1) * width]
            ref[pl.ds(block * per_block, per_block), v] = piece.reshape(per_block, segment, width)

    for j in range(1, lon_count // 2):
        target = lax.rem(lon + 2 * j, lon_count)
        table_copy(tab_ref, lon, target, tab_send.at[0, target]).start()
    table_copy(tab_ref, lon, partner, tab_send.at[0, partner]).start()

    stacked[:, pl.ds(0, width)] = cot_ref[...]
    for v in range(var_count):
        stacked[:, pl.ds((v + 1) * width, width)] = inc_ref[v]

    @pl.loop(0, blocks)
    def _(step):
        block = turn(step)
        rows = pl.ds(pl.multiple_of(block * BLOCK, BLOCK), BLOCK)
        table = pick(column_of(perm_ref[:, rows]) == lane_iota(BLOCK, col_count))
        moved = dot(table, stacked[...]).astype(jnp.bfloat16)
        cot_out[pl.ds(block * per_block, per_block)] = moved[:, :width].reshape(per_block, segment, width)
        split_rows(fields_out, block, moved[:, width:])
        start_block(0, cot_out, cot_in, block)

    @pl.loop(0, blocks)
    def _(step):
        start_block(1, fields_out, fields_in, turn(step))

    cot_in[me] = cot_out[me]
    fields_in[me] = fields_out[me]
    tabs[lon] = tab_ref[...]
    for j in range(1, lon_count // 2):
        source = lax.rem(lon + 2 * j, lon_count)
        table_copy(tabs.at[source], source, source, tab_send.at[0, source]).wait_recv()
        table_copy(tabs.at[source], source, partner, tab_send.at[1, source]).start()
    wait_all(0, cot_in)
    for j in range(lon_count // 2):
        source = lax.rem(partner + 2 * j, lon_count)
        table_copy(tabs.at[source], source, source, tab_send.at[0, source]).wait_recv()
    depth = tab_ref.shape[2]
    for b in range(band_count):
        for v in range(var_count):
            part = tabs[:, b, v].reshape(lon_count * depth, width)
            wide[pl.ds(v * lon_count * depth, lon_count * depth), pl.ds(b * width, width)] = part

    @pl.loop(0, row_count // BLOCK)
    def _(step):
        start = pl.multiple_of(step * BLOCK, BLOCK)
        rows = pl.ds(start, BLOCK)
        spot = row_iota(BLOCK, col_count, start)
        table = blend(back_ref[0:1, :] == spot, back_ref[1:2, :] == spot, back_w[...])
        coarse = dot(table, cot_in[...].reshape(col_count, width))
        scale = jnp.transpose(scale_ref[:, rows])
        lifted = jnp.concatenate([(scale[:, b : b + 1] * coarse).astype(jnp.bfloat16) for b in range(band_count)], axis=1)
        out = lax.dot_general(lifted, wide[...], (((1,), (1,)), ((), ())), preferred_element_type=jnp.float32)
        adj[rows, :] = out.astype(jnp.bfloat16)

    @pl.loop(0, blocks)
    def _(step):
        block = turn(step)
        spot = row_iota(BLOCK, row_count, block * BLOCK)
        table = blend(coarse_ref[0:1, :] == spot, coarse_ref[1:2, :] == spot, coarse_w[...])
        split_rows(grad_out, block, dot(table, adj[...]).astype(jnp.bfloat16))
        start_block(2, grad_out, grad_in, block)

    grad_in[me] = grad_out[me]
    wait_all(1, fields_in)
    for v in range(var_count):
        flat[:, pl.ds(v * width, width)] = fields_in[:, v].reshape(col_count, width)

    @pl.loop(0, row_count // BLOCK)
    def _(step):
        rows = pl.ds(pl.multiple_of(step * BLOCK, BLOCK), BLOCK)
        spot = lane_iota(BLOCK, col_count)
        first, second = column_of(coarse_ref[0:1, rows]), column_of(coarse_ref[1:2, rows])
        table = blend(first == spot, second == spot, column_of(coarse_w[:, rows]))
        coarse = dot(table, flat[...]).astype(jnp.bfloat16)
        scale = jnp.transpose(scale_ref[:, rows])
        total = jnp.zeros((BLOCK, width), jnp.float32)
        for b in range(0, band_count, 2):
            pair = dot(coarse, wide[:, b * width : (b + 2) * width])
            total = total + scale[:, b : b + 1] * pair[:, :width] + scale[:, b + 1 : b + 2] * pair[:, width:]
        heat[rows, :] = total.astype(jnp.bfloat16)

    @pl.loop(0, blocks)
    def _(step):
        block = turn(step)
        rows = pl.ds(pl.multiple_of(block * BLOCK, BLOCK), BLOCK)
        spot = lane_iota(BLOCK, row_count)
        first, second = column_of(back_ref[0:1, rows]), column_of(back_ref[1:2, rows])
        table = blend(first == spot, second == spot, column_of(back_w[:, rows]))
        moved = dot(table, heat[...]).astype(jnp.bfloat16)
        tend_out[pl.ds(block * per_block, per_block)] = moved.reshape(per_block, segment, width)
        start_block(3, tend_out, tend_in, block)

    tend_in[me] = tend_out[me]
    for j in range(1, lon_count // 2):
        other = lax.rem(lon + 2 * j, lon_count)
        table_copy(tab_ref, other, other, tab_send.at[0, other]).wait_send()
        table_copy(tab_ref, other, other, tab_send.at[1, other]).wait_send()
    table_copy(tab_ref, partner, partner, tab_send.at[0, partner]).wait_send()
    wait_all(2, grad_in)
    wait_all(3, tend_in)
    wait_sent(0, cot_out)
    wait_sent(1, fields_out)
    wait_sent(2, grad_out)
    wait_sent(3, tend_out)


def restore_kernel(perm_ref, tend_ref, grad_ref, tend_out, grad_out, stacked):
    devices, var_count, segment, width = grad_ref.shape
    col_count = devices * segment
    stacked[:, pl.ds(0, width)] = tend_ref[...].reshape(col_count, width)
    for v in range(var_count):
        stacked[:, pl.ds((v + 1) * width, width)] = grad_ref[:, v].reshape(col_count, width)

    @pl.loop(0, col_count // BLOCK)
    def one(step):
        rows = pl.ds(pl.multiple_of(step * BLOCK, BLOCK), BLOCK)
        table = pick(perm_ref[...] == row_iota(BLOCK, col_count, step * BLOCK))
        moved = dot(table, stacked[...]).astype(jnp.bfloat16)
        tend_out[rows, :] = moved[:, :width]
        for v in range(var_count):
            grad_out[v, rows, :] = moved[:, (v + 1) * width : (v + 2) * width]


def run(kernel, outs, scratch, flops, args, sems=(), talks=False):
    shapes = [jax.ShapeDtypeStruct(shape, jnp.bfloat16) for shape in outs]
    vmem = pl.BlockSpec(memory_space=pltpu.VMEM)
    return pl.pallas_call(
        kernel,
        out_shape=shapes,
        in_specs=[vmem] * len(args),
        out_specs=[vmem] * len(outs),
        scratch_shapes=[pltpu.VMEM(shape, jnp.bfloat16) for shape in scratch] + [pltpu.SemaphoreType.DMA(shape) for shape in sems],
        compiler_params=pltpu.CompilerParams(vmem_limit_bytes=56 * 1024 * 1024, has_side_effects=talks),
        cost_estimate=pl.CostEstimate(flops=flops, bytes_accessed=4 << 20, transcendentals=0),
    )(*args)


def local(
    increments,
    cotangent,
    owner_perm,
    coarse_index,
    coarse_weight,
    back_index,
    back_weight,
    lw_scale,
    sw_scale,
    sunlit,
    lw_table,
    sw_table,
    *,
    devices,
    lon_count,
):
    table = jnp.concatenate([lw_table, sw_table])
    col_count, var_count, width = increments.shape
    row_count = coarse_weight.shape[0]
    segment = col_count // devices
    thin, split = (devices, segment, width), (devices, var_count, segment, width)
    flat_width = var_count * width
    bands = table.shape[0]
    planes = jnp.transpose(increments, (1, 0, 2))
    stack = (col_count, (var_count + 1) * width)
    move_cost = 2 * col_count * stack[0] * stack[1]
    pad = jnp.zeros((-bands % 8, row_count), jnp.float32)
    scale = jnp.concatenate([lw_scale, sw_scale * sunlit.astype(jnp.float32)[None, :], pad])
    back_w, coarse_w = back_weight[None, :], coarse_weight[None, :]
    back_tend, back_grad = run(
        functools.partial(radiate_kernel, lon_count),
        [thin, split],
        [
            stack,
            thin,
            thin,
            split,
            split,
            split,
            thin,
            (lon_count,) + table.shape,
            (flat_width, bands * width),
            (col_count, flat_width),
            (row_count, flat_width),
            (row_count, width),
        ],
        6 * row_count * bands * flat_width * width,
        (owner_perm, planes, cotangent, back_index, back_w, scale, table, coarse_index, coarse_w),
        sems=((4, devices), (4, devices), (2, lon_count), (lon_count,)),
        talks=True,
    )
    tendency, gradient = run(
        restore_kernel,
        [(col_count, width), (var_count, col_count, width)],
        [stack],
        move_cost,
        (owner_perm, back_tend, back_grad),
    )
    return (tendency, jnp.transpose(gradient, (1, 0, 2)))


def solution(mesh):
    in_specs = (
        P(("lat", "lon"), None, None),
        P(("lat", "lon"), None),
        P(("lat", "lon"), None),
        P(None, ("lat", "lon")),
        P(("lat", "lon")),
        P(None, ("lat", "lon")),
        P(("lat", "lon")),
        P(None, ("lat", "lon")),
        P(None, ("lat", "lon")),
        P(("lat", "lon")),
        P(None, None, "lon", None),
        P(None, None, "lon", None),
    )
    out_specs = (P(("lat", "lon"), None), P(("lat", "lon"), None, None))
    devices = mesh.shape["lat"] * mesh.shape["lon"]

    def body(*args):
        return local(*args, devices=devices, lon_count=mesh.shape["lon"])

    return jax.shard_map(body, mesh=mesh, in_specs=in_specs, out_specs=out_specs, check_vma=False)
```

```python
import functools

import jax
import jax.numpy as jnp
from jax import lax
from jax.experimental import pallas as pl
from jax.experimental.pallas import tpu as pltpu
from jax.sharding import PartitionSpec as P

BLOCK = 256


def lane_iota(rows, width):
    return lax.broadcasted_iota(jnp.int32, (rows, width), 1)


def row_iota(rows, width, start):
    return lax.broadcasted_iota(jnp.int32, (rows, width), 0) + start


def pick(hit):
    return jnp.where(hit, 1.0, 0.0).astype(jnp.bfloat16)


def blend(hit_first, hit_second, share):
    first = jnp.where(hit_first, share, 0.0)
    second = jnp.where(hit_second, 1.0 - share, 0.0)
    return (first + second).astype(jnp.bfloat16)


def dot(left, right):
    return lax.dot_general(left, right, (((1,), (0,)), ((), ())), preferred_element_type=jnp.float32)


def column_of(values):
    return jnp.transpose(jnp.broadcast_to(values, (8, values.shape[1])))[:, 0:1]


def radiate_kernel(
    lon_count,
    perm_ref,
    inc_ref,
    cot_ref,
    back_ref,
    back_w,
    lw_scale,
    sw_scale,
    sun_ref,
    lw_ref,
    sw_ref,
    coarse_ref,
    coarse_w,
    tend_done,
    grad_done,
    tend_in,
    grad_in,
    back,
    stacked,
    cot_out,
    cot_in,
    fields_out,
    fields_in,
    grad_out,
    tend_out,
    tabs,
    wide,
    flat,
    adj,
    heat,
    send_sem,
    recv_sem,
    tab_send,
    tab_recv,
):
    var_count, col_count, width = inc_ref.shape
    devices, segment = cot_out.shape[0], cot_out.shape[1]
    row_count = lw_scale.shape[1]
    lw_count = lw_ref.shape[0]
    band_count = lw_count + sw_ref.shape[0]
    per_block = BLOCK // segment
    blocks = col_count // BLOCK
    lat, lon = lax.axis_index("lat"), lax.axis_index("lon")
    me = lat * lon_count + lon
    parity = lax.rem(lon, 2)
    partner = lon + 1 - 2 * parity
    home = lax.div(me, per_block)

    def table_copy(source, slot, target, sem):
        return pltpu.make_async_remote_copy(
            src_ref=source,
            dst_ref=tabs.at[slot],
            send_sem=sem,
            recv_sem=tab_recv.at[slot],
            device_id=(lat, target),
            device_id_type=pl.DeviceIdType.MESH,
        )

    def copy(kind, source, landing, target, slot):
        return pltpu.make_async_remote_copy(
            src_ref=source,
            dst_ref=landing,
            send_sem=send_sem.at[kind, target],
            recv_sem=recv_sem.at[kind, slot],
            device_id=(lax.div(target, lon_count), lax.rem(target, lon_count)),
            device_id_type=pl.DeviceIdType.MESH,
        )

    def start_block(kind, source, landing, block):
        for k in range(per_block):
            target = block * per_block + k

            @pl.when(target != me)
            def _():
                copy(kind, source.at[target], landing.at[me], target, me).start()

    def wait_all(kind, landing):
        @pl.loop(1, devices)
        def _(k):
            source = lax.rem(me + k, devices)
            copy(kind, landing.at[source], landing.at[source], source, source).wait_recv()

    def wait_sent(kind, source):
        @pl.loop(1, devices)
        def _(k):
            target = lax.rem(me + k, devices)
            copy(kind, source.at[target], source.at[target], target, target).wait_send()

    def scale_of(rows):
        lit = sun_ref[:, rows].astype(jnp.float32)
        longwave, shortwave = jnp.transpose(lw_scale[:, rows]), jnp.transpose(sw_scale[:, rows] * lit)
        return [
            longwave[:, b : b + 1] if b < lw_count else shortwave[:, b - lw_count : b - lw_count + 1]
            for b in range(band_count)
        ]

    def turn(step):
        return lax.rem(step + home + 1, blocks)

    def split_rows(ref, block, values):
        for v in range(var_count):
            piece = values[:, v * width : (v + 1) * width]
            ref[pl.ds(block * per_block, per_block), v] = piece.reshape(per_block, segment, width)

    tabs[lon, pl.ds(0, lw_count)] = lw_ref[...]
    tabs[lon, pl.ds(lw_count, band_count - lw_count)] = sw_ref[...]
    stacked[:, pl.ds(0, width)] = cot_ref[...]
    for v in range(var_count):
        stacked[:, pl.ds((v + 1) * width, width)] = inc_ref[v]

    for j in range(1, lon_count // 2):
        target = lax.rem(lon + 2 * j, lon_count)
        table_copy(tabs.at[lon], lon, target, tab_send.at[0, target]).start()
    table_copy(tabs.at[lon], lon, partner, tab_send.at[0, partner]).start()

    @pl.loop(0, blocks)
    def _(step):
        block = turn(step)
        rows = pl.ds(pl.multiple_of(block * BLOCK, BLOCK), BLOCK)
        table = pick(column_of(perm_ref[:, rows]) == lane_iota(BLOCK, col_count))
        moved = dot(table, stacked[...]).astype(jnp.bfloat16)
        cot_out[pl.ds(block * per_block, per_block)] = moved[:, :width].reshape(per_block, segment, width)
        split_rows(fields_out, block, moved[:, width:])
        start_block(0, cot_out, cot_in, block)

    @pl.loop(0, blocks)
    def _(step):
        start_block(1, fields_out, fields_in, turn(step))

    cot_in[me] = cot_out[me]
    fields_in[me] = fields_out[me]
    for j in range(1, lon_count // 2):
        source = lax.rem(lon + 2 * j, lon_count)
        table_copy(tabs.at[source], source, source, tab_send.at[0, source]).wait_recv()
        table_copy(tabs.at[source], source, partner, tab_send.at[1, source]).start()
    wait_all(0, cot_in)
    for j in range(lon_count // 2):
        source = lax.rem(partner + 2 * j, lon_count)
        table_copy(tabs.at[source], source, source, tab_send.at[0, source]).wait_recv()
    depth = lw_ref.shape[2]
    for b in range(band_count):
        for v in range(var_count):
            part = tabs[:, b, v].reshape(lon_count * depth, width)
            wide[pl.ds(v * lon_count * depth, lon_count * depth), pl.ds(b * width, width)] = part

    @pl.loop(0, row_count // BLOCK)
    def _(step):
        start = pl.multiple_of(step * BLOCK, BLOCK)
        rows = pl.ds(start, BLOCK)
        spot = row_iota(BLOCK, col_count, start)
        table = blend(back_ref[0:1, :] == spot, back_ref[1:2, :] == spot, back_w[...])
        coarse = dot(table, cot_in[...].reshape(col_count, width))
        scale = scale_of(rows)
        lifted = jnp.concatenate([(scale[b] * coarse).astype(jnp.bfloat16) for b in range(band_count)], axis=1)
        out = lax.dot_general(lifted, wide[...], (((1,), (1,)), ((), ())), preferred_element_type=jnp.float32)
        adj[rows, :] = out.astype(jnp.bfloat16)

    @pl.loop(0, blocks)
    def _(step):
        block = turn(step)
        spot = row_iota(BLOCK, row_count, block * BLOCK)
        table = blend(coarse_ref[0:1, :] == spot, coarse_ref[1:2, :] == spot, coarse_w[...])
        split_rows(grad_out, block, dot(table, adj[...]).astype(jnp.bfloat16))
        start_block(2, grad_out, grad_in, block)

    grad_in[me] = grad_out[me]

    @pl.loop(0, blocks)
    def _(step):
        start = pl.multiple_of(step * BLOCK, BLOCK)
        back[pl.ds(start, BLOCK), :] = pick(perm_ref[...] == row_iota(BLOCK, col_count, start))

    wait_all(1, fields_in)
    for v in range(var_count):
        flat[:, pl.ds(v * width, width)] = fields_in[:, v].reshape(col_count, width)

    @pl.loop(0, row_count // BLOCK)
    def _(step):
        rows = pl.ds(pl.multiple_of(step * BLOCK, BLOCK), BLOCK)
        spot = lane_iota(BLOCK, col_count)
        first, second = column_of(coarse_ref[0:1, rows]), column_of(coarse_ref[1:2, rows])
        table = blend(first == spot, second == spot, column_of(coarse_w[:, rows]))
        coarse = dot(table, flat[...]).astype(jnp.bfloat16)
        scale = scale_of(rows)
        total = jnp.zeros((BLOCK, width), jnp.float32)
        for b in range(0, band_count, 2):
            pair = dot(coarse, wide[:, b * width : (b + 2) * width])
            total = total + scale[b] * pair[:, :width] + scale[b + 1] * pair[:, width:]
        heat[rows, :] = total.astype(jnp.bfloat16)

    @pl.loop(0, blocks)
    def _(step):
        block = turn(step)
        rows = pl.ds(pl.multiple_of(block * BLOCK, BLOCK), BLOCK)
        spot = lane_iota(BLOCK, row_count)
        first, second = column_of(back_ref[0:1, rows]), column_of(back_ref[1:2, rows])
        table = blend(first == spot, second == spot, column_of(back_w[:, rows]))
        moved = dot(table, heat[...]).astype(jnp.bfloat16)
        tend_out[pl.ds(block * per_block, per_block)] = moved.reshape(per_block, segment, width)
        start_block(3, tend_out, tend_in, block)

    tend_in[me] = tend_out[me]
    for j in range(1, lon_count // 2):
        other = lax.rem(lon + 2 * j, lon_count)
        table_copy(tabs.at[lon], other, other, tab_send.at[0, other]).wait_send()
        table_copy(tabs.at[lon], other, other, tab_send.at[1, other]).wait_send()
    table_copy(tabs.at[lon], partner, partner, tab_send.at[0, partner]).wait_send()
    wait_all(2, grad_in)
    for v in range(var_count):
        flat[:, pl.ds(v * width, width)] = grad_in[:, v].reshape(col_count, width)

    @pl.loop(0, blocks)
    def _(step):
        rows = pl.ds(pl.multiple_of(step * BLOCK, BLOCK), BLOCK)
        moved = dot(back[rows, :], flat[...]).astype(jnp.bfloat16)
        for v in range(var_count):
            grad_done[v, rows, :] = moved[:, v * width : (v + 1) * width]

    wait_all(3, tend_in)

    @pl.loop(0, blocks)
    def _(step):
        rows = pl.ds(pl.multiple_of(step * BLOCK, BLOCK), BLOCK)
        tend_done[rows, :] = dot(back[rows, :], tend_in[...].reshape(col_count, width)).astype(jnp.bfloat16)

    wait_sent(0, cot_out)
    wait_sent(1, fields_out)
    wait_sent(2, grad_out)
    wait_sent(3, tend_out)


def run(kernel, outs, scratch, flops, args, sems=(), talks=False):
    shapes = [jax.ShapeDtypeStruct(shape, jnp.bfloat16) for shape in outs]
    vmem = pl.BlockSpec(memory_space=pltpu.VMEM)
    return pl.pallas_call(
        kernel,
        out_shape=shapes,
        in_specs=[vmem] * len(args),
        out_specs=[vmem] * len(outs),
        scratch_shapes=[pltpu.VMEM(shape, jnp.bfloat16) for shape in scratch] + [pltpu.SemaphoreType.DMA(shape) for shape in sems],
        compiler_params=pltpu.CompilerParams(vmem_limit_bytes=56 * 1024 * 1024, has_side_effects=talks),
        cost_estimate=pl.CostEstimate(flops=flops, bytes_accessed=4 << 20, transcendentals=0),
    )(*args)


def local(
    increments,
    cotangent,
    owner_perm,
    coarse_index,
    coarse_weight,
    back_index,
    back_weight,
    lw_scale,
    sw_scale,
    sunlit,
    lw_table,
    sw_table,
    *,
    devices,
    lon_count,
):
    col_count, var_count, width = increments.shape
    row_count = coarse_weight.shape[0]
    segment = col_count // devices
    thin, split = (devices, segment, width), (devices, var_count, segment, width)
    flat_width = var_count * width
    bands = lw_table.shape[0] + sw_table.shape[0]
    planes = jnp.transpose(increments, (1, 0, 2))
    stack = (col_count, (var_count + 1) * width)
    back_w, coarse_w = back_weight[None, :], coarse_weight[None, :]
    tendency, gradient = run(
        functools.partial(radiate_kernel, lon_count),
        [(col_count, width), (var_count, col_count, width)],
        [
            thin,
            split,
            (col_count, col_count),
            stack,
            thin,
            thin,
            split,
            split,
            split,
            thin,
            (lon_count, bands) + lw_table.shape[1:],
            (flat_width, bands * width),
            (col_count, flat_width),
            (row_count, flat_width),
            (row_count, width),
        ],
        6 * row_count * bands * flat_width * width,
        (
            owner_perm,
            planes,
            cotangent,
            back_index,
            back_w,
            lw_scale,
            sw_scale,
            sunlit[None, :],
            lw_table,
            sw_table,
            coarse_index,
            coarse_w,
        ),
        sems=((4, devices), (4, devices), (2, lon_count), (lon_count,)),
        talks=True,
    )
    return (tendency, jnp.transpose(gradient, (1, 0, 2)))


def solution(mesh):
    in_specs = (
        P(("lat", "lon"), None, None),
        P(("lat", "lon"), None),
        P(("lat", "lon"), None),
        P(None, ("lat", "lon")),
        P(("lat", "lon")),
        P(None, ("lat", "lon")),
        P(("lat", "lon")),
        P(None, ("lat", "lon")),
        P(None, ("lat", "lon")),
        P(("lat", "lon")),
        P(None, None, "lon", None),
        P(None, None, "lon", None),
    )
    out_specs = (P(("lat", "lon"), None), P(("lat", "lon"), None, None))
    devices = mesh.shape["lat"] * mesh.shape["lon"]

    def body(*args):
        return local(*args, devices=devices, lon_count=mesh.shape["lon"])

    return jax.shard_map(body, mesh=mesh, in_specs=in_specs, out_specs=out_specs, check_vma=False)
```
